32 devices in a mesh: env: 4 (over y, core), dof: 8 (over z, x).
Axes of the slice: x: 2, y: 2, z: 4, core: 2. Of those that a mesh axis runs over, the one named last changes fastest.
Arguments:
- system_matrix: bfloat16 [8, 8192, 8192], P('env', 'dof'), parts along dimension 0, as said below
- forces: float32 [8192, 8, 128], P('dof', 'env'), parts along dimension 1, may hold values from -6 to 6
Outputs:
- accelerations: float32 [8192, 8, 128], P('dof', 'env'), parts along dimension 1
- residual: float32 [8192, 8, 128], P('dof', 'env'), parts along dimension 1
The draws below stay inside these ranges and needn't reach their ends.
There are 4 independent parts, one for each index of `env`. The reference program is written for one: setup_inputs(seed, part) draws one part's arguments, and reference() takes and returns one part's arrays. A program takes and returns all parts, laid end to end along the dimension named above; each array names one. Nothing has to cross between parts.
Inputs may be any that keep to these rules, and one draw needn't show every extreme that they name: `system_matrix`: each environment's matrix is exactly symmetric and positive definite.
All inputs are finite; a program needn't handle non-finite values.
Results may differ from the reference program's by a relative error of at most 0.012.
Values may be sent and summed in bfloat16 or wider, within the bound.
A program may use at most 128 MiB of HBM per device.

```python
import jax
import jax.numpy as jnp
from jax import lax

N = 8192
ENVS = 2
RHS = 128
ITERS = 4


def draw_system_matrix(key, part):
    key_noise = jax.random.fold_in(key, 21)
    key_scale = jax.random.fold_in(key, 22)
    key_shift = jax.random.fold_in(key, 23)
    scales = jnp.exp(jax.random.uniform(key_scale, (ENVS, N), jnp.float32, 0.0, 1.1513))
    shift = jax.random.uniform(key_shift, (ENVS, N), jnp.float32, 0.2, 0.5)

    def one_matrix(index):
        factor = jax.random.normal(jax.random.fold_in(key_noise, index), (N, N), jnp.float32)
        gram = jnp.dot(factor, factor.T, precision=lax.Precision.HIGHEST) * (1.0 / N)
        gram = 0.5 * (gram + gram.T)
        gram = gram + jnp.diag(shift[index])
        outer = scales[index][:, None] * scales[index][None, :]
        return (gram * outer).astype(jnp.bfloat16)
    return lax.map(one_matrix, jnp.arange(ENVS, dtype=jnp.int32))


def levels(stream_key, dims, cuts, least, high):
    level, own = 1.0, jax.random.fold_in(stream_key, 6)
    for dim, blocks in cuts:
        heights = jnp.exp(jax.random.uniform(jax.random.fold_in(own, dim), (blocks,), jnp.float32, least / len(cuts), high / len(cuts)))
        level = level * jnp.repeat(heights, dims[dim] // blocks).reshape([-1 if axis == dim else 1 for axis in range(len(dims))])
    return level


def gaussian(key, dims, scale, reach, pieces=(), kind=jnp.bfloat16):
    array = jax.random.normal(key, dims, jnp.float32) * scale
    if len(pieces) > 0:
        array = levels(key, dims, pieces, -0.22, 0.18) * array
    return jnp.clip(array, min=-reach, max=reach).astype(kind)


def setup_inputs(seed: int = 0, part: int = 0) -> dict:
    splits = jax.random.split(jax.random.key(seed), 3)
    own_keys = jax.random.split(jax.random.fold_in(splits[2], part), 3)
    return {
        "system_matrix": draw_system_matrix(jax.random.fold_in(jax.random.fold_in(splits[2], part), 71), part),
        "forces": gaussian(own_keys[1], (N, ENVS, RHS), 1.0, 6.0, ((0, 8),), jnp.float32),
    }


def apply_matrix(system_matrix, field):
    narrow = field.astype(jnp.bfloat16)
    columns = [jnp.dot(system_matrix[index], narrow[:, index, :], preferred_element_type=jnp.float32) for index in range(ENVS)]
    return jnp.stack(columns, axis=1)


def reference(system_matrix, forces):
    accelerations = jnp.zeros_like(forces)
    residual = forces
    direction = forces
    norm_now = jnp.sum(residual * residual, axis=0)
    for step in range(ITERS):
        image = apply_matrix(system_matrix, direction)
        alpha = norm_now / jnp.sum(direction * image, axis=0)
        accelerations = accelerations + alpha * direction
        residual = residual - alpha * image
        norm_next = jnp.sum(residual * residual, axis=0)
        direction = residual + (norm_next / norm_now) * direction
        norm_now = norm_next
    return accelerations, residual
```

```python
import functools

import jax
import jax.numpy as jnp
from jax import lax
from jax.experimental import pallas as pl
from jax.experimental.pallas import tpu as pltpu
from jax.sharding import PartitionSpec as P

ITERS = 4
MESH = pl.DeviceIdType.MESH


def ring_order(n):
    width = 1
    while (2 * width) ** 2 <= n:
        width *= 2
    depth = n // width
    if width == 1 or depth % 2:
        return list(range(n))
    order = [z * width for z in range(depth)]
    for turn, z in enumerate(reversed(range(depth))):
        xs = list(range(1, width))
        order += [z * width + x for x in (xs if turn % 2 == 0 else xs[::-1])]
    return order


def lookup(table, index):
    value = jnp.int32(0)
    for place, entry in enumerate(table):
        value = value + jnp.where(index == place, jnp.int32(entry), jnp.int32(0))
    return value


def kernel(n, envs, rows, a_hbm, f_ref, x_ref, r_ref, a_vmem, field, direction, image, sums,
           load_sem, send_sem, recv_sem, sum_send, sum_recv):
    order = ring_order(n)
    inverse = [order.index(i) for i in range(n)]
    me = lax.axis_index("dof")
    place = lookup(inverse, me)
    half = rows // 2
    far = n // 2
    tile = min(128, rows)

    def owner(step):
        return lookup(order, lax.rem(place + step + n, n))

    following, previous = owner(1), owner(-1)

    def load(env, block):
        return pltpu.make_async_copy(
            a_hbm.at[env, :, pl.ds(pl.multiple_of(block * rows, rows), rows)],
            a_vmem.at[env, block],
            load_sem.at[env, block],
        )

    def hop(env, way, block, part, target):
        return pltpu.make_async_remote_copy(
            src_ref=field.at[env, block, part],
            dst_ref=field.at[env, block, part],
            send_sem=send_sem.at[env, way, block, part],
            recv_sem=recv_sem.at[env, block, part],
            device_id={"dof": target},
            device_id_type=MESH,
        )

    def forward(env, block, part):
        return hop(env, 0, block, part, following)

    def backward(env, block, part):
        return hop(env, 1, block, part, previous)

    def share(env, slot, peer, source):
        return pltpu.make_async_remote_copy(
            src_ref=sums.at[env, slot, source],
            dst_ref=sums.at[env, slot, source],
            send_sem=sum_send.at[env, slot, peer],
            recv_sem=sum_recv.at[env, slot, source],
            device_id={"dof": peer},
            device_id_type=MESH,
        )

    def peer_of(j):
        return lax.rem(me + j, n)

    def add(env, block, part, first=False):
        product = jnp.dot(
            a_vmem[env, block, :, part * half:(part + 1) * half],
            field[env, block, part],
            preferred_element_type=jnp.float32,
        )
        if first:
            image[env] = product
        else:
            image[env] += product

    def start_own(env):
        for q in range(2):
            forward(env, me, q).start()
            backward(env, me, 1 - q).start()

    def begin(env, k):
        @pl.when(k == 0)
        def _():
            load(env, me).wait()
        add(env, me, 0, first=True)
        add(env, me, 1)

    def near(env, k, s, relay):
        before, after = owner(-s), owner(s)
        for q in range(2):
            forward(env, before, q).wait_recv()
            if relay > q:
                forward(env, before, q).start()
            backward(env, after, 1 - q).wait_recv()
            if relay > q:
                backward(env, after, 1 - q).start()
            if q == 0:
                @pl.when(k == 0)
                def _():
                    load(env, before).wait()
                    load(env, after).wait()
            if relay == 1 and q == 0:
                yield
            add(env, before, q)
            add(env, after, 1 - q)

    def gather(env, k, between):
        begin(env, k)

        def step(s, carry):
            for _ in near(env, k, s, 2):
                pass
            return carry

        lax.fori_loop(1, far - 1, step, 0)
        for _ in near(env, k, far - 1, 1):
            between()
        block = owner(far)
        forward(env, block, 0).wait_recv()

        @pl.when(k == 0)
        def _():
            load(env, block).wait()
        add(env, block, 0)
        backward(env, block, 1).wait_recv()
        add(env, block, 1)

        def drain(s, carry):
            for q in range(2):
                forward(env, owner(-s), q).wait_send()
                backward(env, owner(s), q).wait_send()
            return carry

        lax.fori_loop(0, far - 1, drain, 0)
        forward(env, owner(1 - far), 0).wait_send()
        backward(env, owner(far - 1), 1).wait_send()

    def local_sums(env, k):
        slot = lax.rem(k, 2)

        def step(i, carry):
            at = pl.ds(pl.multiple_of(i * tile, tile), tile)
            r, d, q = r_ref[env, at, :], direction[env, at, :], image[env, at, :]
            fold = lambda v: jnp.sum(v.reshape(tile // 8, 8, v.shape[-1]), axis=0)
            return tuple(c + fold(v) for c, v in zip(carry, (r * r, d * q, r * q, q * q)))

        zero = jnp.zeros((8, image.shape[-1]), jnp.float32)
        totals = lax.fori_loop(0, rows // tile, step, (zero,) * 4)
        for i, total in enumerate(totals):
            sums[env, slot, me, i:i + 1, :] = jnp.sum(total, axis=0, keepdims=True)

        def send(j, carry):
            share(env, slot, peer_of(j), me).start()
            return carry

        lax.fori_loop(1, n, send, 0)

    def update(env, k):
        slot = lax.rem(k, 2)

        def receive(j, carry):
            share(env, slot, me, peer_of(j)).wait_recv()
            share(env, slot, peer_of(j), me).wait_send()
            return carry

        lax.fori_loop(1, n, receive, 0)
        total = sums[env, slot, 0]
        for j in range(1, n):
            total = total + sums[env, slot, j]
        now, curve, cross, square = (total[i:i + 1, :] for i in range(4))
        alpha = now / curve
        beta = (now - 2.0 * alpha * cross + alpha * alpha * square) / now

        def step(i, carry):
            at = pl.ds(pl.multiple_of(i * tile, tile), tile)
            d = direction[env, at, :]
            x_ref[env, at, :] = x_ref[env, at, :] + alpha * d
            r = r_ref[env, at, :] - alpha * image[env, at, :]
            r_ref[env, at, :] = r
            d = r + beta * d
            direction[env, at, :] = d
            put(env, i, d)
            return carry

        lax.fori_loop(0, rows // tile, step, 0)

    def put(env, i, d):
        per = half // tile if half >= tile else 1
        narrow = d.astype(field.dtype)
        if half >= tile:
            at = pl.ds(pl.multiple_of(lax.rem(i, per) * tile, tile), tile)
            field[env, me, i // per, at, :] = narrow
        else:
            for q in range(2):
                field[env, me, q] = narrow[q * half:(q + 1) * half]

    barrier = pltpu.get_barrier_semaphore()

    def greet(j, carry):
        pl.semaphore_signal(barrier, inc=1, device_id={"dof": peer_of(j)}, device_id_type=MESH)
        return carry

    def copy_in(env):
        def step(i, carry):
            at = pl.ds(pl.multiple_of(i * tile, tile), tile)
            f = f_ref[env, at, :]
            x_ref[env, at, :] = jnp.zeros_like(f)
            r_ref[env, at, :] = f
            direction[env, at, :] = f
            put(env, i, f)
            return carry
        lax.fori_loop(0, rows // tile, step, 0)

    lax.fori_loop(1, n, greet, 0)
    copy_in(0)
    for env in range(envs):
        load(env, me).start()

        def fetch(s, carry):
            load(env, owner(-s)).start()
            load(env, owner(s)).start()
            return carry

        lax.fori_loop(1, far, fetch, 0)
        load(env, owner(far)).start()
    pl.semaphore_wait(barrier, n - 1)
    start_own(0)
    copy_in(1)

    def iteration(k, carry):
        def second():
            @pl.when(k > 0)
            def _():
                update(1, k - 1)
            start_own(1)

        def first():
            update(0, k)

            @pl.when(k < ITERS - 1)
            def _():
                start_own(0)

        gather(0, k, second)
        local_sums(0, k)
        gather(1, k, first)
        local_sums(1, k)
        return carry

    lax.fori_loop(0, ITERS, iteration, 0)
    update(1, ITERS - 1)


def solution(mesh):
    n = mesh.shape["dof"]

    def on_device(system_matrix, forces):
        envs, rows, _ = system_matrix.shape
        rhs = forces.shape[-1]
        block = jax.ShapeDtypeStruct((envs, rows, rhs), jnp.float32)
        vmem = pl.BlockSpec(memory_space=pltpu.VMEM)
        x, r = pl.pallas_call(
            functools.partial(kernel, n, envs, rows),
            out_shape=(block, block),
            in_specs=[pl.BlockSpec(memory_space=pl.ANY), vmem],
            out_specs=(vmem, vmem),
            scratch_shapes=[
                pltpu.VMEM((envs, n, rows, rows), jnp.bfloat16),
                pltpu.VMEM((envs, n, 2, rows // 2, rhs), jnp.bfloat16),
                pltpu.VMEM((envs, rows, rhs), jnp.float32),
                pltpu.VMEM((envs, rows, rhs), jnp.float32),
                pltpu.VMEM((envs, 2, n, 4, rhs), jnp.float32),
                pltpu.SemaphoreType.DMA((envs, n)),
                pltpu.SemaphoreType.DMA((envs, 2, n, 2)),
                pltpu.SemaphoreType.DMA((envs, n, 2)),
                pltpu.SemaphoreType.DMA((envs, 2, n)),
                pltpu.SemaphoreType.DMA((envs, 2, n)),
            ],
            compiler_params=pltpu.CompilerParams(
                collective_id=0, has_side_effects=True, vmem_limit_bytes=60 * 1024 * 1024
            ),
        )(system_matrix, forces.transpose(1, 0, 2))
        return x.transpose(1, 0, 2), r.transpose(1, 0, 2)

    return jax.shard_map(
        on_device,
        mesh=mesh,
        in_specs=(P("env", "dof", None), P("dof", "env", None)),
        out_specs=(P("dof", "env", None), P("dof", "env", None)),
        check_vma=False,
    )
```
